256 devices in a mesh: row: 8 (over x, z_lo), col: 32 (over z_hi, y, core).
Axes of the slice: x: 4, y: 4, z: 8 (z_hi: 4, z_lo: 2; z = z_hi * 2 + z_lo), core: 2. Of those that a mesh axis runs over, the one named last changes fastest.
Arguments:
- tile_values: float32 [8, 32, 64, 128, 128], P('row', 'col'), may hold values from -0.15625 to 0.15625
- tile_rows: int32 [8, 32, 64], P('row', 'col'), may hold values from 0 to 159, as said below
- tile_cols: int32 [8, 32, 64], P('row', 'col'), may hold values from 0 to 23
- x_start: float32 [768, 128], P('col', 'row'), may hold values from -6 to 6
- z_start: float32 [1280, 128], P('row'), may hold values from -6 to 6
- y_start: float32 [1280, 128], P('row'), may hold values from -3 to 3
- lower_bound: float32 [1280, 128], P('row'), may hold values from -1.5 to -0.1
- upper_bound: float32 [1280, 128], P('row'), may hold values from 0.1 to 1.5
- cost_diag: float32 [768, 128], P('col', 'row'), may hold values from 0.1 to 10
- linear: float32 [768, 128], P('col', 'row'), may hold values from -6 to 6
- penalty: float32 [1], replicated, may hold values from 0.3 to 3
- proximal: float32 [1], replicated, may hold values from 0.1 to 1
- relaxation: float32 [1], replicated, may hold values from 1.2 to 1.8
Outputs:
- x_next: float32 [768, 128], P('col', 'row')
- z_next: float32 [1280, 128], P('row')
- y_next: float32 [1280, 128], P('row')
The draws below stay inside these ranges and needn't reach their ends.
Inputs may be any that keep to these rules, and one draw needn't show every extreme that they name: On each device the 64 pairs (tile_rows, tile_cols) are distinct.
All inputs are finite; a program needn't handle non-finite values.
Results may differ from the reference program's by a relative error of at most 0.0002.
Values sent between devices are 32-bit elements; how exact they have to be, the bound alone decides.
A program may use at most 64 MiB of HBM per device.

```python
import math
import jax
import jax.numpy as jnp
from jax import lax

BS = 128
XB = 24
ZB = 160
TPD = 64
ADMM_ITERS = 2
CG_STEPS = 1
NB = 768
MB = 1280
N_ROW = 8
N_COL = 32


def tile_pattern(key):
    folded = jax.random.fold_in(key, 7)
    subkeys = jax.random.split(folded, N_ROW * N_COL)
    chosen = jax.vmap(lambda subkey: jax.random.permutation(subkey, ZB * XB)[:TPD])(subkeys)
    chosen = chosen.reshape(N_ROW, N_COL, TPD).astype(jnp.int32)
    return (chosen // XB, chosen % XB)


def draw_tile_rows(key, part):
    return tile_pattern(key)[0]


def draw_tile_cols(key, part):
    return tile_pattern(key)[1]


def steps_of(rng, extent, cuts, smallest, high):
    def one(dim, shards_of):
        heights = jax.random.uniform(jax.random.fold_in(jax.random.fold_in(rng, 6), dim), (shards_of,), jnp.float32, smallest / len(cuts), high / len(cuts))
        return jnp.repeat(jnp.exp(heights), extent[dim] // shards_of).reshape((-1,) + (1,) * (len(extent) - dim - 1))

    factor_of = one(*cuts[0])
    for cut in cuts[1:]:
        factor_of = factor_of * one(*cut)
    return factor_of


def scatter_about(own_key, shape, width, most, cuts=(), kind=jnp.bfloat16):
    drawn = jax.random.normal(own_key, shape, jnp.float32) * width
    if len(cuts) > 0:
        drawn = steps_of(own_key, shape, cuts, -0.22, 0.18) * drawn
    return jnp.clip(drawn, min=-most, max=most).astype(kind)


def setup_inputs(seed: int = 0) -> dict:
    keys = jax.random.split(jax.random.key(seed), 14)
    tile_values = scatter_about(keys[0], (N_ROW, N_COL, TPD, BS, BS), (BS * TPD * N_COL // ZB) ** -0.5, 0.15625, ((0, 8), (1, 32)), jnp.float32)
    tile_rows = draw_tile_rows(jax.random.fold_in(keys[13], 71), 0)
    tile_cols = draw_tile_cols(jax.random.fold_in(keys[13], 71), 0)
    x_start = scatter_about(keys[3], (NB, BS), 1.0, 6.0, ((0, 32), (1, 8)), jnp.float32)
    z_start = scatter_about(keys[4], (MB, BS), 1.0, 6.0, ((0, 8),), jnp.float32)
    y_start = scatter_about(keys[5], (MB, BS), 0.5, 3.0, ((0, 8),), jnp.float32)
    lower_bound = jnp.clip(-1.5 + 1.4 * jax.random.uniform(keys[6], (MB, BS), jnp.float32) ** steps_of(keys[6], (MB, BS), ((0, 8),), -0.2, 0.2), -1.5, -0.1)
    upper_bound = jnp.clip(0.1 + 1.4 * jax.random.uniform(keys[7], (MB, BS), jnp.float32) ** steps_of(keys[7], (MB, BS), ((0, 8),), -0.2, 0.2), 0.1, 1.5)
    cost_diag = jnp.clip(jnp.exp(math.log(10.0) - 4.6051702 * jax.random.uniform(keys[8], (NB, BS), jnp.float32) ** steps_of(keys[8], (NB, BS), ((0, 32), (1, 8)), -0.2, 0.2)), 0.1, 10.0)
    linear = scatter_about(keys[9], (NB, BS), 1.0, 6.0, ((0, 32), (1, 8)), jnp.float32)
    penalty = jnp.clip(jnp.exp(jax.random.uniform(keys[10], (1,), jnp.float32, math.log(0.3), math.log(3.0))), 0.3, 3.0)
    proximal = jnp.clip(jnp.exp(jax.random.uniform(keys[11], (1,), jnp.float32, math.log(0.1), math.log(1.0))), 0.1, 1.0)
    relaxation = jnp.clip(jax.random.uniform(keys[12], (1,), jnp.float32, 1.2, 1.8), 1.2, 1.8)
    return {"tile_values": tile_values, "tile_rows": tile_rows, "tile_cols": tile_cols, "x_start": x_start, "z_start": z_start, "y_start": y_start, "lower_bound": lower_bound, "upper_bound": upper_bound, "cost_diag": cost_diag, "linear": linear, "penalty": penalty, "proximal": proximal, "relaxation": relaxation}


HIGH = lax.Precision.HIGHEST


def block_indices(tile_rows, tile_cols):
    row_base = jnp.arange(N_ROW, dtype=jnp.int32)[:, None, None] * ZB
    col_base = jnp.arange(N_COL, dtype=jnp.int32)[None, :, None] * XB
    return (tile_rows + row_base).reshape(-1), (tile_cols + col_base).reshape(-1)


def forward_apply(flat_tiles, global_rows, global_cols, vector):
    picked = jnp.take(vector, global_cols, axis=0)
    products = jnp.einsum("kij,kj->ki", flat_tiles, picked, precision=HIGH)
    return jax.ops.segment_sum(products, global_rows, num_segments=MB)


def backward_apply(flat_tiles, global_rows, global_cols, weights_rows):
    picked = jnp.take(weights_rows, global_rows, axis=0)
    products = jnp.einsum("kij,ki->kj", flat_tiles, picked, precision=HIGH)
    return jax.ops.segment_sum(products, global_cols, num_segments=NB)


def reference(tile_values, tile_rows, tile_cols, x_start, z_start, y_start, lower_bound, upper_bound, cost_diag, linear, penalty, proximal, relaxation):
    flat_tiles = tile_values.reshape(-1, BS, BS)
    global_rows, global_cols = block_indices(tile_rows, tile_cols)
    rho_value = penalty[0]
    sigma_value = proximal[0]
    relax_value = relaxation[0]
    x_now, z_now, y_now = x_start, z_start, y_start
    for outer_round in range(ADMM_ITERS):
        image_now = forward_apply(flat_tiles, global_rows, global_cols, x_now)
        target = rho_value * z_now - y_now - rho_value * image_now
        residual = -linear - cost_diag * x_now + backward_apply(flat_tiles, global_rows, global_cols, target)
        guess = x_now
        direction = residual
        norm_now = jnp.sum(residual * residual)
        for inner_round in range(CG_STEPS):
            pushed = forward_apply(flat_tiles, global_rows, global_cols, direction)
            applied = (cost_diag + sigma_value) * direction + rho_value * backward_apply(flat_tiles, global_rows, global_cols, pushed)
            step_length = norm_now / jnp.sum(direction * applied)
            guess = guess + step_length * direction
            residual = residual - step_length * applied
            norm_next = jnp.sum(residual * residual)
            direction = residual + (norm_next / norm_now) * direction
            norm_now = norm_next
        z_tilde = forward_apply(flat_tiles, global_rows, global_cols, guess)
        x_now = relax_value * guess + (1.0 - relax_value) * x_now
        mixed = relax_value * z_tilde + (1.0 - relax_value) * z_now
        z_fresh = jnp.minimum(jnp.maximum(mixed + y_now / rho_value, lower_bound), upper_bound)
        y_now = y_now + rho_value * (mixed - z_fresh)
        z_now = z_fresh
    return x_now, z_now, y_now
```

```python
import functools

import jax
import jax.numpy as jnp
from jax import lax
from jax.experimental import pallas as pl
from jax.experimental.pallas import tpu as pltpu
from jax.sharding import PartitionSpec as P

ITERS = 2
MESH = pl.DeviceIdType.MESH
F32 = jnp.float32


def pieces(value, count):
    out = []
    for _ in range(count - 1):
        head = value.astype(jnp.bfloat16).astype(F32)
        out.append(head)
        value = value - head
    out.append(value)
    return out


def select(table, value, count):
    return sum(jnp.dot(table, part, preferred_element_type=F32) for part in pieces(value, count))


def kernel(
    dims,
    rho_ref,
    sigma_ref,
    relax_ref,
    rows_ref,
    cols_ref,
    x0_ref,
    diag0_ref,
    lin0_ref,
    z0_ref,
    y0_ref,
    low0_ref,
    high0_ref,
    tiles_hbm,
    x_out,
    z_out,
    y_out,
    tiles,
    turned,
    acc,
    row_pick,
    row_sum,
    col_pick,
    col_sum,
    zs,
    ys,
    low,
    high,
    image,
    xs,
    diag,
    lin,
    start_buf,
    back_buf,
    part_buf,
    rs_buf,
    ar_buf,
    ag_buf,
    srow_buf,
    scol_buf,
    load_sem,
    start_send,
    start_recv,
    back_send,
    back_recv,
    rs_send,
    rs_recv,
    ar_send,
    ar_recv,
    ag_send,
    ag_recv,
    srow_send,
    srow_recv,
    scol_send,
    scol_recv,
):
    n_row, n_hi, n_lo, xb, zb, pad, width = dims
    count = tiles.shape[0]
    lanes = tiles.shape[2]
    piece = zb // n_lo
    row = lax.axis_index("row")
    col = lax.axis_index("col")
    hi = lax.div(col, n_lo)
    lo = lax.rem(col, n_lo)

    def row_peer(step):
        other = lax.rem(row + step, n_row)
        return other, (other, col)

    def hi_peer(step):
        other = lax.rem(hi + step, n_hi)
        return other, (row, other * n_lo + lo)

    def lo_peer(step):
        other = lax.rem(lo + step, n_lo)
        return other, (row, hi * n_lo + other)

    groups = ((n_row, row_peer), (n_hi, hi_peer), (n_lo, lo_peer))

    barrier = pltpu.get_barrier_semaphore()
    for size, peer in groups:
        for step in range(1, size):
            pl.semaphore_signal(barrier, inc=1, device_id=peer(step)[1], device_id_type=MESH)

    load = pltpu.make_async_copy(tiles_hbm, tiles, load_sem)
    load.start()

    def exchange(size, peer, source, target, mine, send_sem, recv_sem):
        for step in range(1, size):
            other, device = peer(step)
            pltpu.make_async_remote_copy(
                src_ref=source(other),
                dst_ref=target(mine),
                send_sem=send_sem(other),
                recv_sem=recv_sem(mine),
                device_id=device,
                device_id_type=MESH,
            ).start()

    def arrive(size, peer, source, target, send_sem, recv_sem):
        for step in range(1, size):
            other, device = peer(step)
            copy = pltpu.make_async_remote_copy(
                src_ref=source(other),
                dst_ref=target(other),
                send_sem=send_sem(other),
                recv_sem=recv_sem(other),
                device_id=device,
                device_id_type=MESH,
            )
            copy.wait_recv()
            copy.wait_send()

    start_buf[row] = jnp.concatenate(
        [x0_ref[...], diag0_ref[...], lin0_ref[...], jnp.zeros((xb, lanes - 3 * width), F32)], axis=1
    )

    rows = rows_ref[...]
    padded = rows
    for k in range(1, n_lo):
        padded = padded + jnp.where(rows >= k * piece, pad - piece, 0)
    table = (lax.broadcasted_iota(jnp.int32, (n_lo * pad, count), 0) == padded).astype(F32)
    row_pick[...] = table.T
    spread = (
        lax.broadcasted_iota(jnp.int32, (count, 8 * count), 0)
        == lax.broadcasted_iota(jnp.int32, (count, 8 * count), 1) // 8
    ).astype(F32)
    row_sum[...] = jnp.dot(table, spread, preferred_element_type=F32)
    table = (lax.broadcasted_iota(jnp.int32, (xb, count), 0) == cols_ref[...]).astype(F32)
    col_pick[...] = table.T
    col_sum[...] = jnp.dot(table, spread, preferred_element_type=F32)

    pl.semaphore_wait(barrier, sum(size - 1 for size, _ in groups))

    start_args = (lambda other: start_buf.at[row], lambda slot: start_buf.at[slot])
    start_sems = (lambda k: start_send.at[k], lambda k: start_recv.at[k])
    exchange(n_row, row_peer, *start_args, row, *start_sems)

    for ref, source in ((zs, z0_ref), (ys, y0_ref), (low, low0_ref), (high, high0_ref)):
        ref[...] = jnp.zeros_like(ref)
        for k in range(n_lo):
            ref[k, 0:piece, :] = source[k * piece : (k + 1) * piece, :]

    load.wait()
    for k in range(count):
        turned[k] = tiles[k].T

    rho = rho_ref[0]
    sigma = sigma_ref[0]
    relax = relax_ref[0]

    def products(picked, which):
        columns = picked.T
        for k in range(count):
            terms = which[k] * columns[:, k : k + 1]
            acc[8 * k : 8 * k + 8, :] = jnp.sum(terms.reshape(lanes // 8, 8, lanes), axis=0)
        return acc[...]

    def forward(vector, scalars, turn):
        part = select(row_sum[...], products(select(col_pick[...], vector, 3), turned), 2)
        part_buf[turn] = part.reshape(n_lo, pad, lanes)
        for k, value in enumerate(scalars):
            for slot in range(n_lo):
                part_buf[turn, slot, piece + k : piece + k + 1, :] = value
        rs_buf[turn, lo] = part_buf[turn, lo]
        rs_args = (lambda other: part_buf.at[turn, other], lambda slot: rs_buf.at[turn, slot])
        rs_sems = (lambda k: rs_send.at[turn, k], lambda k: rs_recv.at[turn, k])
        exchange(n_lo, lo_peer, *rs_args, lo, *rs_sems)
        yield
        arrive(n_lo, lo_peer, *rs_args, *rs_sems)
        ar_buf[turn, hi] = sum(rs_buf[turn, k] for k in range(n_lo))
        ar_args = (lambda other: ar_buf.at[turn, hi], lambda slot: ar_buf.at[turn, slot])
        ar_sems = (lambda k: ar_send.at[turn, k], lambda k: ar_recv.at[turn, k])
        exchange(n_hi, hi_peer, *ar_args, hi, *ar_sems)
        yield
        arrive(n_hi, hi_peer, *ar_args, *ar_sems)
        whole = sum(ar_buf[turn, k] for k in range(n_hi))
        inside = lax.broadcasted_iota(jnp.int32, whole.shape, 0) < piece
        kept = jnp.where(inside, whole, 0.0)
        ag_buf[turn, lo] = kept
        ag_args = (lambda other: ag_buf.at[turn, lo], lambda slot: ag_buf.at[turn, slot])
        ag_sems = (lambda k: ag_send.at[turn, k], lambda k: ag_recv.at[turn, k])
        exchange(n_lo, lo_peer, *ag_args, lo, *ag_sems)
        yield kept, [whole[piece + k : piece + k + 1, :] for k in range(len(scalars))]
        arrive(n_lo, lo_peer, *ag_args, *ag_sems)
        yield

    arrive(n_row, row_peer, *start_args, *start_sems)
    lane = lax.broadcasted_iota(jnp.int32, (xb, lanes), 1)
    for index, ref in enumerate((xs, diag, lin)):
        total = jnp.zeros((xb, lanes), F32)
        for k in range(n_row):
            moved = pltpu.roll(start_buf[k], (width * (k - index)) % lanes, axis=1)
            total = jnp.where((lane >= width * k) & (lane < width * (k + 1)), moved, total)
        ref[...] = total

    for _ in forward(xs[...], [], 0):
        pass
    image[...] = ag_buf[0]

    def iteration(turn, carry):
        target = rho * zs[...] - ys[...] - rho * image[...]
        target = target.reshape(n_lo * pad, lanes)
        back_buf[turn, row] = select(col_sum[...], products(select(row_pick[...], target, 3), tiles), 2)
        back_args = (lambda other: back_buf.at[turn, row], lambda slot: back_buf.at[turn, slot])
        back_sems = (lambda k: back_send.at[turn, k], lambda k: back_recv.at[turn, k])
        exchange(n_row, row_peer, *back_args, row, *back_sems)
        local = -lin[...] - diag[...] * xs[...]
        arrive(n_row, row_peer, *back_args, *back_sems)
        residual = local + sum(back_buf[turn, k] for k in range(n_row))

        square = residual * residual
        norm = jnp.sum(square, axis=0, keepdims=True)
        bend = jnp.sum((diag[...] + sigma) * square, axis=0, keepdims=True)
        stages = forward(residual, [norm, bend], turn + 1)
        next(stages)
        next(stages)
        kept, (norm, bend) = next(stages)

        srow_buf[turn, row] = jnp.sum(kept * kept, axis=0, keepdims=True)
        srow_args = (lambda other: srow_buf.at[turn, row], lambda slot: srow_buf.at[turn, slot])
        srow_sems = (lambda k: srow_send.at[turn, k], lambda k: srow_recv.at[turn, k])
        exchange(n_row, row_peer, *srow_args, row, *srow_sems)
        arrive(n_row, row_peer, *srow_args, *srow_sems)
        scol_buf[turn, lo] = sum(srow_buf[turn, k] for k in range(n_row))
        scol_args = (lambda other: scol_buf.at[turn, lo], lambda slot: scol_buf.at[turn, slot])
        scol_sems = (lambda k: scol_send.at[turn, k], lambda k: scol_recv.at[turn, k])
        exchange(n_lo, lo_peer, *scol_args, lo, *scol_sems)
        next(stages)
        arrive(n_lo, lo_peer, *scol_args, *scol_sems)
        bend = bend + rho * sum(scol_buf[turn, k] for k in range(n_lo))

        step = jnp.sum(norm, axis=1, keepdims=True) / jnp.sum(bend, axis=1, keepdims=True)
        x_now = xs[...]
        xs[...] = relax * (x_now + step * residual) + (1.0 - relax) * x_now
        for k in range(n_lo):
            old = image[k]
            moved = old + step * ag_buf[turn + 1, k]
            image[k] = relax * moved + (1.0 - relax) * old
            mixed = relax * moved + (1.0 - relax) * zs[k]
            y_now = ys[k]
            z_new = jnp.minimum(jnp.maximum(mixed + y_now / rho, low[k]), high[k])
            ys[k] = y_now + rho * (mixed - z_new)
            zs[k] = z_new
        return carry

    lax.fori_loop(0, ITERS, iteration, 0)

    x_out[...] = pltpu.roll(xs[...], lax.rem(lanes - width * row, lanes), axis=1)[:, :width]
    for k in range(n_lo):
        z_out[k * piece : (k + 1) * piece, :] = zs[k, 0:piece, :]
        y_out[k * piece : (k + 1) * piece, :] = ys[k, 0:piece, :]


def solution(mesh):
    n_row, n_col = mesh.shape["row"], mesh.shape["col"]
    n_lo = 8
    n_hi = n_col // n_lo

    def shards(values, rows, cols, x0, z0, y0, low0, high0, diag0, lin0, rho, sigma, relax):
        order = values.shape[-1]
        tiles = values.reshape(-1, order, order)
        count = tiles.shape[0]
        zb, lanes = z0.shape
        xb, width = x0.shape
        piece = zb // n_lo
        pad = (piece + 2 + 7) // 8 * 8
        dims = (n_row, n_hi, n_lo, xb, zb, pad, width)
        smem = pl.BlockSpec(memory_space=pltpu.SMEM)
        vmem = pl.BlockSpec(memory_space=pltpu.VMEM)
        dma = pltpu.SemaphoreType.DMA
        wide = (n_lo, pad, lanes)
        return pl.pallas_call(
            functools.partial(kernel, dims),
            out_shape=(
                jax.ShapeDtypeStruct(x0.shape, F32),
                jax.ShapeDtypeStruct(z0.shape, F32),
                jax.ShapeDtypeStruct(z0.shape, F32),
            ),
            in_specs=[smem] * 3 + [vmem] * 9 + [pl.BlockSpec(memory_space=pl.ANY)],
            out_specs=(vmem, vmem, vmem),
            scratch_shapes=[
                pltpu.VMEM((count, order, order), F32),
                pltpu.VMEM((count, order, order), F32),
                pltpu.VMEM((8 * count, lanes), F32),
                pltpu.VMEM((count, n_lo * pad), F32),
                pltpu.VMEM((n_lo * pad, 8 * count), F32),
                pltpu.VMEM((count, xb), F32),
                pltpu.VMEM((xb, 8 * count), F32),
                *[pltpu.VMEM(wide, F32)] * 5,
                *[pltpu.VMEM((xb, lanes), F32)] * 3,
                pltpu.VMEM((n_row, xb, lanes), F32),
                pltpu.VMEM((ITERS, n_row, xb, lanes), F32),
                pltpu.VMEM((ITERS + 1, *wide), F32),
                pltpu.VMEM((ITERS + 1, *wide), F32),
                pltpu.VMEM((ITERS + 1, n_hi, pad, lanes), F32),
                pltpu.VMEM((ITERS + 1, *wide), F32),
                pltpu.VMEM((ITERS, n_row, 1, lanes), F32),
                pltpu.VMEM((ITERS, n_lo, 1, lanes), F32),
                dma(()),
                dma((n_row,)),
                dma((n_row,)),
                dma((ITERS, n_row)),
                dma((ITERS, n_row)),
                dma((ITERS + 1, n_lo)),
                dma((ITERS + 1, n_lo)),
                dma((ITERS + 1, n_hi)),
                dma((ITERS + 1, n_hi)),
                dma((ITERS + 1, n_lo)),
                dma((ITERS + 1, n_lo)),
                dma((ITERS, n_row)),
                dma((ITERS, n_row)),
                dma((ITERS, n_lo)),
                dma((ITERS, n_lo)),
            ],
            compiler_params=pltpu.CompilerParams(collective_id=0, has_side_effects=True),
            name="admm",
        )(rho, sigma, relax, rows.reshape(1, -1), cols.reshape(1, -1), x0, diag0, lin0, z0, y0, low0, high0, tiles)

    placed = (
        P("row", "col", None, None, None),
        P("row", "col", None),
        P("row", "col", None),
        P("col", "row"),
        P("row", None),
        P("row", None),
        P("row", None),
        P("row", None),
        P("col", "row"),
        P("col", "row"),
        P(),
        P(),
        P(),
    )
    return jax.shard_map(
        shards,
        mesh=mesh,
        in_specs=placed,
        out_specs=(P("col", "row"), P("row", None), P("row", None)),
        check_vma=False,
    )
```

```python
import functools

import jax
import jax.numpy as jnp
from jax import lax
from jax.experimental import pallas as pl
from jax.experimental.pallas import tpu as pltpu
from jax.sharding import PartitionSpec as P

ITERS = 2
MESH = pl.DeviceIdType.MESH
F32 = jnp.float32
BF16 = jnp.bfloat16


def pieces(value, count):
    out = []
    for _ in range(count - 1):
        head = value.astype(BF16)
        out.append(head)
        value = value - head.astype(F32)
    out.append(value.astype(BF16))
    return out


def select(table, value):
    return sum(jnp.dot(table, part, preferred_element_type=F32) for part in pieces(value, 2))


def kernel(
    dims,
    rho_hbm,
    sigma_hbm,
    relax_hbm,
    rows_hbm,
    cols_hbm,
    x0_hbm,
    diag0_hbm,
    lin0_hbm,
    z0_hbm,
    y0_hbm,
    low0_hbm,
    high0_hbm,
    tiles_hbm,
    out,
    rho_ref,
    sigma_ref,
    relax_ref,
    rows_ref,
    cols_ref,
    index_buf,
    small_buf,
    plain_buf,
    tiles,
    turned,
    acc,
    picked,
    vector_buf,
    row_sum,
    col_sum,
    zs,
    ys,
    low,
    high,
    image,
    xs,
    diag,
    lin,
    start_buf,
    cost_buf,
    back_buf,
    part_buf,
    rs_buf,
    ar_buf,
    ag_buf,
    norm_buf,
    load_sem,
    start_send,
    start_recv,
    cost_send,
    cost_recv,
    back_send,
    back_recv,
    rs_send,
    rs_recv,
    ar_send,
    ar_recv,
    ag_send,
    ag_recv,
    norm_send,
    norm_recv,
):
    n_row, n_hi, n_lo, xb, zb, pad, width = dims
    count = tiles.shape[0]
    lanes = tiles.shape[2]
    piece = zb // n_lo
    row = lax.axis_index("row")
    col = lax.axis_index("col")
    hi = lax.div(col, n_lo)
    lo = lax.rem(col, n_lo)

    def row_peer(step):
        other = lax.rem(row + step, n_row)
        return other, (other, col)

    def hi_peer(step):
        other = lax.rem(hi + step, n_hi)
        return other, (row, other * n_lo + lo)

    def lo_peer(step):
        other = lax.rem(lo + step, n_lo)
        return other, (row, hi * n_lo + other)

    def plane_peer(step):
        other_row = lax.rem(row + step // n_lo, n_row)
        other_lo = lax.rem(lo + step % n_lo, n_lo)
        return other_row * n_lo + other_lo, (other_row, hi * n_lo + other_lo)

    n_plane = n_row * n_lo
    plane = row * n_lo + lo

    barrier = pltpu.get_barrier_semaphore()
    for size, peer in ((n_plane, plane_peer), (n_hi, hi_peer)):
        for step in range(1, size):
            pl.semaphore_signal(barrier, inc=1, device_id=peer(step)[1], device_id_type=MESH)

    loads = [
        pltpu.make_async_copy(source, target, load_sem.at[k])
        for k, (source, target) in enumerate(
            (
                (x0_hbm, small_buf.at[0]),
                (diag0_hbm, small_buf.at[1]),
                (lin0_hbm, small_buf.at[2]),
                (rows_hbm, index_buf.at[0]),
                (cols_hbm, index_buf.at[1]),
                (rows_hbm, rows_ref),
                (cols_hbm, cols_ref),
                (rho_hbm, rho_ref),
                (sigma_hbm, sigma_ref),
                (relax_hbm, relax_ref),
                (z0_hbm, plain_buf.at[0]),
                (y0_hbm, plain_buf.at[1]),
                (low0_hbm, plain_buf.at[2]),
                (high0_hbm, plain_buf.at[3]),
                (tiles_hbm, tiles),
            )
        )
    ]
    for load in loads:
        load.start()

    def exchange(size, peer, source, target, mine, send_sem, recv_sem):
        for step in range(1, size):
            other, device = peer(step)
            pltpu.make_async_remote_copy(
                src_ref=source(other),
                dst_ref=target(mine),
                send_sem=send_sem(other),
                recv_sem=recv_sem(mine),
                device_id=device,
                device_id_type=MESH,
            ).start()

    def arrive(size, peer, source, target, send_sem, recv_sem):
        for step in range(1, size):
            other, device = peer(step)
            copy = pltpu.make_async_remote_copy(
                src_ref=source(other),
                dst_ref=target(other),
                send_sem=send_sem(other),
                recv_sem=recv_sem(other),
                device_id=device,
                device_id_type=MESH,
            )
            copy.wait_recv()
            copy.wait_send()

    empty = jnp.zeros((width, lanes - xb), F32)
    for load in loads[:5]:
        load.wait()
    start_buf[row] = jnp.concatenate([small_buf[0], empty], axis=1)
    for k in range(2):
        cost_buf[row, k] = jnp.concatenate([small_buf[k + 1], empty], axis=1)

    rows = index_buf[0]
    padded = rows
    for k in range(1, n_lo):
        padded = padded + jnp.where(rows >= k * piece, pad - piece, 0)
    row_sum[...] = (lax.broadcasted_iota(jnp.int32, (n_lo * pad, count), 0) == padded).astype(BF16)
    col_sum[...] = (lax.broadcasted_iota(jnp.int32, (xb, count), 0) == index_buf[1]).astype(BF16)
    for load in loads[5:10]:
        load.wait()

    pl.semaphore_wait(barrier, n_plane - 1 + n_hi - 1)

    start_args = (lambda other: start_buf.at[row], lambda slot: start_buf.at[slot])
    start_sems = (lambda k: start_send.at[k], lambda k: start_recv.at[k])
    exchange(n_row, row_peer, *start_args, row, *start_sems)
    cost_args = (lambda other: cost_buf.at[row], lambda slot: cost_buf.at[slot])
    cost_sems = (lambda k: cost_send.at[k], lambda k: cost_recv.at[k])
    exchange(n_row, row_peer, *cost_args, row, *cost_sems)

    for load in loads[10:]:
        load.wait()
    for k in range(count):
        turned[k] = tiles[k].T
    for index, ref in enumerate((zs, ys, low, high)):
        ref[...] = jnp.zeros_like(ref)
        for k in range(n_lo):
            ref[k, 0:piece, :] = plain_buf[index, k * piece : (k + 1) * piece, :]

    rho = rho_ref[0]
    sigma = sigma_ref[0]
    relax = relax_ref[0]

    def products(which):
        columns = picked[...].T
        for k in range(count):
            terms = which[k] * columns[:, k : k + 1]
            acc[k : k + 1, :] = jnp.sum(terms, axis=0, keepdims=True)
        return acc[...]

    def forward(vector, scalars, turn):
        vector_buf[0:xb, :] = vector
        for k in range(count):
            picked[k : k + 1, :] = vector_buf[pl.ds(cols_ref[0, k], 1), :]
        part = select(row_sum[...], products(turned))
        part_buf[turn] = part.reshape(n_lo, pad, lanes)
        for k, value in enumerate(scalars):
            for slot in range(n_lo):
                part_buf[turn, slot, piece + k : piece + k + 1, :] = value
        rs_buf[turn, lo] = part_buf[turn, lo]
        rs_args = (lambda other: part_buf.at[turn, other], lambda slot: rs_buf.at[turn, slot])
        rs_sems = (lambda k: rs_send.at[turn, k], lambda k: rs_recv.at[turn, k])
        exchange(n_lo, lo_peer, *rs_args, lo, *rs_sems)
        yield
        arrive(n_lo, lo_peer, *rs_args, *rs_sems)
        ar_buf[turn, hi] = sum(rs_buf[turn, k] for k in range(n_lo))
        ar_args = (lambda other: ar_buf.at[turn, hi], lambda slot: ar_buf.at[turn, slot])
        ar_sems = (lambda k: ar_send.at[turn, k], lambda k: ar_recv.at[turn, k])
        exchange(n_hi, hi_peer, *ar_args, hi, *ar_sems)
        yield
        arrive(n_hi, hi_peer, *ar_args, *ar_sems)
        whole = sum(ar_buf[turn, k] for k in range(n_hi))
        inside = lax.broadcasted_iota(jnp.int32, whole.shape, 0) < piece
        kept = jnp.where(inside, whole, 0.0)
        ag_buf[turn, lo] = kept
        ag_args = (lambda other: ag_buf.at[turn, lo], lambda slot: ag_buf.at[turn, slot])
        ag_sems = (lambda k: ag_send.at[turn, k], lambda k: ag_recv.at[turn, k])
        if scalars:
            norm_buf[turn - 1, plane] = jnp.sum(kept * kept, axis=0, keepdims=True)
            exchange(n_plane, plane_peer, *norm_args(turn - 1), plane, *norm_sems(turn - 1))
        exchange(n_lo, lo_peer, *ag_args, lo, *ag_sems)
        yield [whole[piece + k : piece + k + 1, :] for k in range(len(scalars))]
        arrive(n_lo, lo_peer, *ag_args, *ag_sems)
        yield

    def norm_args(turn):
        return lambda other: norm_buf.at[turn, plane], lambda slot: norm_buf.at[turn, slot]

    def norm_sems(turn):
        return lambda k: norm_send.at[turn, k], lambda k: norm_recv.at[turn, k]

    arrive(n_row, row_peer, *start_args, *start_sems)
    xs[...] = jnp.concatenate([start_buf[k] for k in range(n_row)], axis=0).T[:xb]
    stages = forward(xs[...], [], 0)
    next(stages)
    arrive(n_row, row_peer, *cost_args, *cost_sems)
    diag[...] = jnp.concatenate([cost_buf[k, 0] for k in range(n_row)], axis=0).T[:xb]
    lin[...] = jnp.concatenate([cost_buf[k, 1] for k in range(n_row)], axis=0).T[:xb]
    for _ in stages:
        pass
    image[...] = ag_buf[0]

    def iteration(turn, carry):
        for k in range(n_lo):
            vector_buf[k * pad : (k + 1) * pad, :] = rho * zs[k] - ys[k] - rho * image[k]
        for k in range(count):
            index = rows_ref[0, k]
            index = index + (pad - piece) * (index // piece)
            picked[k : k + 1, :] = vector_buf[pl.ds(index, 1), :]
        back_buf[turn, row] = select(col_sum[...], products(tiles))
        back_args = (lambda other: back_buf.at[turn, row], lambda slot: back_buf.at[turn, slot])
        back_sems = (lambda k: back_send.at[turn, k], lambda k: back_recv.at[turn, k])
        exchange(n_row, row_peer, *back_args, row, *back_sems)
        local = -lin[...] - diag[...] * xs[...]
        arrive(n_row, row_peer, *back_args, *back_sems)
        residual = local + sum(back_buf[turn, k] for k in range(n_row))

        square = residual * residual
        norm = jnp.sum(square, axis=0, keepdims=True)
        bend = jnp.sum((diag[...] + sigma) * square, axis=0, keepdims=True)
        stages = forward(residual, [norm, bend], turn + 1)
        next(stages)
        next(stages)
        norm, bend = next(stages)
        next(stages)
        arrive(n_plane, plane_peer, *norm_args(turn), *norm_sems(turn))
        bend = bend + rho * jnp.sum(norm_buf[turn], axis=0)

        step = jnp.sum(norm, axis=1, keepdims=True) / jnp.sum(bend, axis=1, keepdims=True)
        x_now = xs[...]
        xs[...] = relax * (x_now + step * residual) + (1.0 - relax) * x_now
        for k in range(n_lo):
            old = image[k]
            moved = old + step * ag_buf[turn + 1, k]
            image[k] = relax * moved + (1.0 - relax) * old
            mixed = relax * moved + (1.0 - relax) * zs[k]
            y_now = ys[k]
            z_new = jnp.minimum(jnp.maximum(mixed + y_now / rho, low[k]), high[k])
            ys[k] = y_now + rho * (mixed - z_new)
            zs[k] = z_new
        return carry

    lax.fori_loop(0, ITERS, iteration, 0)

    for k in range(n_lo):
        out[k * piece : (k + 1) * piece, :] = zs[k, 0:piece, :]
        out[zb + k * piece : zb + (k + 1) * piece, :] = ys[k, 0:piece, :]
    mine = pltpu.roll(xs[...], lax.rem(lanes - width * row, lanes), axis=1)
    out[2 * zb : 2 * zb + xb, :] = mine


def unpack(packed, x_out, z_out, y_out):
    zb = z_out.shape[0]
    width, xb = x_out.shape
    z_out[...] = packed[0:zb, :]
    y_out[...] = packed[zb : 2 * zb, :]
    x_out[...] = packed[2 * zb : 2 * zb + xb, :].T[:width]


def solution(mesh):
    n_row, n_col = mesh.shape["row"], mesh.shape["col"]
    n_lo = 8
    n_hi = n_col // n_lo

    def shards(values, rows, cols, x0, z0, y0, low0, high0, diag0, lin0, rho, sigma, relax):
        order = values.shape[-1]
        tiles = values.reshape(-1, order, order)
        count = tiles.shape[0]
        zb, lanes = z0.shape
        xb, width = x0.shape
        piece = zb // n_lo
        pad = (piece + 2 + 7) // 8 * 8
        dims = (n_row, n_hi, n_lo, xb, zb, pad, width)
        smem = pltpu.SMEM
        vmem = pltpu.VMEM
        dma = pltpu.SemaphoreType.DMA
        wide = (n_lo, pad, lanes)
        packed = pl.pallas_call(
            functools.partial(kernel, dims),
            out_shape=jax.ShapeDtypeStruct((2 * zb + xb, lanes), F32),
            in_specs=[pl.BlockSpec(memory_space=pltpu.HBM)] * 13,
            out_specs=pl.BlockSpec(memory_space=pltpu.VMEM),
            scratch_shapes=[
                smem((1,), F32),
                smem((1,), F32),
                smem((1,), F32),
                smem((1, count), jnp.int32),
                smem((1, count), jnp.int32),
                vmem((2, 1, count), jnp.int32),
                vmem((3, width, xb), F32),
                vmem((4, zb, lanes), F32),
                vmem((count, order, order), F32),
                vmem((count, order, order), F32),
                vmem((count, lanes), F32),
                vmem((count, lanes), F32),
                vmem((n_lo * pad, lanes), F32),
                vmem((n_lo * pad, count), BF16),
                vmem((xb, count), BF16),
                *[vmem(wide, F32)] * 5,
                *[vmem((xb, lanes), F32)] * 3,
                vmem((n_row, width, lanes), F32),
                vmem((n_row, 2, width, lanes), F32),
                vmem((ITERS, n_row, xb, lanes), F32),
                vmem((ITERS + 1, *wide), F32),
                vmem((ITERS + 1, *wide), F32),
                vmem((ITERS + 1, n_hi, pad, lanes), F32),
                vmem((ITERS + 1, *wide), F32),
                vmem((ITERS, n_row * n_lo, 1, lanes), F32),
                dma((15,)),
                dma((n_row,)),
                dma((n_row,)),
                dma((n_row,)),
                dma((n_row,)),
                dma((ITERS, n_row)),
                dma((ITERS, n_row)),
                dma((ITERS + 1, n_lo)),
                dma((ITERS + 1, n_lo)),
                dma((ITERS + 1, n_hi)),
                dma((ITERS + 1, n_hi)),
                dma((ITERS + 1, n_lo)),
                dma((ITERS + 1, n_lo)),
                dma((ITERS, n_row * n_lo)),
                dma((ITERS, n_row * n_lo)),
            ],
            compiler_params=pltpu.CompilerParams(collective_id=0, has_side_effects=True),
            name="admm",
        )(
            rho, sigma, relax, rows.reshape(1, -1), cols.reshape(1, -1),
            x0.T, diag0.T, lin0.T, z0, y0, low0, high0, tiles,
        )
        x_new, z_new, y_new = pl.pallas_call(
            unpack,
            out_shape=(
                jax.ShapeDtypeStruct((width, xb), F32),
                jax.ShapeDtypeStruct((zb, lanes), F32),
                jax.ShapeDtypeStruct((zb, lanes), F32),
            ),
            name="unpack",
        )(packed)
        return x_new.T, z_new, y_new

    placed = (
        P("row", "col", None, None, None),
        P("row", "col", None),
        P("row", "col", None),
        P("col", "row"),
        P("row", None),
        P("row", None),
        P("row", None),
        P("row", None),
        P("col", "row"),
        P("col", "row"),
        P(),
        P(),
        P(),
    )
    return jax.shard_map(
        shards,
        mesh=mesh,
        in_specs=placed,
        out_specs=(P("col", "row"), P("row", None), P("row", None)),
        check_vma=False,
    )
```

```python
import functools

import jax
import jax.numpy as jnp
from jax import lax
from jax.experimental import pallas as pl
from jax.experimental.pallas import tpu as pltpu
from jax.sharding import PartitionSpec as P

ITERS = 2
MESH = pl.DeviceIdType.MESH
F32 = jnp.float32
BF16 = jnp.bfloat16


def pieces(value, count):
    out = []
    for _ in range(count - 1):
        head = value.astype(BF16)
        out.append(head)
        value = value - head.astype(F32)
    out.append(value.astype(BF16))
    return out


def select(table, value):
    return sum(jnp.dot(table, part, preferred_element_type=F32) for part in pieces(value, 2))


def kernel(
    dims,
    rho_ref,
    sigma_ref,
    relax_ref,
    rows_hbm,
    cols_hbm,
    x0_hbm,
    diag0_hbm,
    lin0_hbm,
    z0_hbm,
    y0_hbm,
    low0_hbm,
    high0_hbm,
    tiles_hbm,
    out,
    rows_ref,
    cols_ref,
    index_buf,
    small_buf,
    plain_buf,
    tiles,
    turned,
    acc,
    picked,
    vector_buf,
    row_sum,
    col_sum,
    zs,
    ys,
    low,
    high,
    image,
    xs,
    diag,
    lin,
    start_buf,
    cost_buf,
    back_buf,
    part_buf,
    rs_buf,
    ar_buf,
    ag_buf,
    norm_buf,
    load_sem,
    start_send,
    start_recv,
    cost_send,
    cost_recv,
    back_send,
    back_recv,
    rs_send,
    rs_recv,
    ar_send,
    ar_recv,
    ag_send,
    ag_recv,
    norm_send,
    norm_recv,
):
    n_row, n_hi, n_lo, xb, zb, pad, width = dims
    count = tiles.shape[0]
    lanes = tiles.shape[2]
    piece = zb // n_lo
    row = lax.axis_index("row")
    col = lax.axis_index("col")
    hi = lax.div(col, n_lo)
    lo = lax.rem(col, n_lo)

    def row_peer(step):
        other = lax.rem(row + step, n_row)
        return other, (other, col)

    def hi_peer(step):
        other = lax.rem(hi + step, n_hi)
        return other, (row, other * n_lo + lo)

    def lo_peer(step):
        other = lax.rem(lo + step, n_lo)
        return other, (row, hi * n_lo + other)

    def plane_peer(step):
        other_row = lax.rem(row + step // n_lo, n_row)
        other_lo = lax.rem(lo + step % n_lo, n_lo)
        return other_row * n_lo + other_lo, (other_row, hi * n_lo + other_lo)

    n_plane = n_row * n_lo
    plane = row * n_lo + lo

    barrier = pltpu.get_barrier_semaphore()
    for size, peer in ((n_plane, plane_peer), (n_hi, hi_peer)):
        for step in range(1, size):
            pl.semaphore_signal(barrier, inc=1, device_id=peer(step)[1], device_id_type=MESH)

    smalls = [(x0_hbm, small_buf.at[0], 0), (diag0_hbm, small_buf.at[1], 0), (lin0_hbm, small_buf.at[2], 0)]
    indices = [(rows_hbm, index_buf.at[0], 1), (cols_hbm, index_buf.at[1], 1), (rows_hbm, rows_ref, 2), (cols_hbm, cols_ref, 3)]
    plains = [(ref, plain_buf.at[k], 4) for k, ref in enumerate((z0_hbm, y0_hbm, low0_hbm, high0_hbm))]
    for source, target, k in [*smalls, *indices, *plains, (tiles_hbm, tiles, 5)]:
        pltpu.make_async_copy(source, target, load_sem.at[k]).start()

    def loaded(k, target):
        pltpu.make_async_copy(target, target, load_sem.at[k]).wait()

    def exchange(size, peer, source, buffer, mine, send_sem, recv_sem):
        for step in range(1, size):
            other, device = peer(step)
            pltpu.make_async_remote_copy(
                src_ref=source(other),
                dst_ref=buffer.at[mine],
                send_sem=send_sem,
                recv_sem=recv_sem,
                device_id=device,
                device_id_type=MESH,
            ).start()

    def arrive(size, peer, source, buffer, mine, send_sem, recv_sem):
        every = buffer.at[pl.ds(0, size - 1)]
        copies = pltpu.make_async_remote_copy(
            src_ref=every,
            dst_ref=every,
            send_sem=send_sem,
            recv_sem=recv_sem,
            device_id=peer(1)[1],
            device_id_type=MESH,
        )
        copies.wait_recv()
        copies.wait_send()

    empty = jnp.zeros((width, lanes - xb), F32)
    loaded(0, small_buf)
    loaded(1, index_buf)
    start_buf[row] = jnp.concatenate([small_buf[0], empty], axis=1)
    for k in range(2):
        cost_buf[row, k] = jnp.concatenate([small_buf[k + 1], empty], axis=1)

    rows = index_buf[0]
    padded = rows
    for k in range(1, n_lo):
        padded = padded + jnp.where(rows >= k * piece, pad - piece, 0)
    row_sum[...] = (lax.broadcasted_iota(jnp.int32, (n_lo * pad, count), 0) == padded).astype(BF16)
    col_sum[...] = (lax.broadcasted_iota(jnp.int32, (xb, count), 0) == index_buf[1]).astype(BF16)
    loaded(2, rows_ref)
    loaded(3, cols_ref)

    pl.semaphore_wait(barrier, n_plane - 1 + n_hi - 1)

    start = (n_row, row_peer, lambda other: start_buf.at[row], start_buf, row, start_send, start_recv)
    exchange(*start)
    cost = (n_row, row_peer, lambda other: cost_buf.at[row], cost_buf, row, cost_send, cost_recv)
    exchange(*cost)

    loaded(4, plain_buf)
    loaded(5, tiles)
    for k in range(count):
        turned[k] = tiles[k].T
    for index, ref in enumerate((zs, ys, low, high)):
        ref[...] = jnp.zeros_like(ref)
        for k in range(n_lo):
            ref[k, 0:piece, :] = plain_buf[index, k * piece : (k + 1) * piece, :]

    rho = rho_ref[0]
    sigma = sigma_ref[0]
    relax = relax_ref[0]

    def products(which):
        columns = picked[...].T
        for k in range(count):
            terms = which[k] * columns[:, k : k + 1]
            acc[k : k + 1, :] = jnp.sum(terms, axis=0, keepdims=True)
        return acc[...]

    def forward(vector, scalars, turn):
        vector_buf[0:xb, :] = vector
        for k in range(count):
            picked[k : k + 1, :] = vector_buf[pl.ds(cols_ref[0, k], 1), :]
        part = select(row_sum[...], products(turned))
        part_buf[turn] = part.reshape(n_lo, pad, lanes)
        for k, value in enumerate(scalars):
            for slot in range(n_lo):
                part_buf[turn, slot, piece + k : piece + k + 1, :] = value
        rs_buf[turn, lo] = part_buf[turn, lo]
        parts = part_buf.at[turn]
        scatter = (n_lo, lo_peer, lambda other: parts.at[other], rs_buf.at[turn], lo, rs_send.at[turn], rs_recv.at[turn])
        exchange(*scatter)
        yield
        arrive(*scatter)
        ar_buf[turn, hi] = sum(rs_buf[turn, k] for k in range(n_lo))
        sums = ar_buf.at[turn]
        reduce = (n_hi, hi_peer, lambda other: sums.at[hi], sums, hi, ar_send.at[turn], ar_recv.at[turn])
        exchange(*reduce)
        yield
        arrive(*reduce)
        whole = sum(ar_buf[turn, k] for k in range(n_hi))
        inside = lax.broadcasted_iota(jnp.int32, whole.shape, 0) < piece
        kept = jnp.where(inside, whole, 0.0)
        ag_buf[turn, lo] = kept
        wholes = ag_buf.at[turn]
        gather = (n_lo, lo_peer, lambda other: wholes.at[lo], wholes, lo, ag_send.at[turn], ag_recv.at[turn])
        exchange(*gather)
        if scalars:
            norm_buf[turn - 1, plane] = jnp.sum(kept * kept, axis=0, keepdims=True)
            exchange(*norms(turn - 1))
        yield [whole[piece + k : piece + k + 1, :] for k in range(len(scalars))]
        arrive(*gather)
        yield

    def norms(turn):
        buffer = norm_buf.at[turn]
        return n_plane, plane_peer, lambda other: buffer.at[plane], buffer, plane, norm_send.at[turn], norm_recv.at[turn]

    arrive(*start)
    xs[...] = jnp.concatenate([start_buf[k] for k in range(n_row)], axis=0).T[:xb]
    stages = forward(xs[...], [], 0)
    next(stages)
    arrive(*cost)
    diag[...] = jnp.concatenate([cost_buf[k, 0] for k in range(n_row)], axis=0).T[:xb]
    lin[...] = jnp.concatenate([cost_buf[k, 1] for k in range(n_row)], axis=0).T[:xb]
    for _ in stages:
        pass
    image[...] = ag_buf[0]

    def iteration(turn, carry):
        for k in range(n_lo):
            vector_buf[k * pad : (k + 1) * pad, :] = rho * zs[k] - ys[k] - rho * image[k]
        for k in range(count):
            index = rows_ref[0, k]
            index = index + (pad - piece) * (index // piece)
            picked[k : k + 1, :] = vector_buf[pl.ds(index, 1), :]
        back_buf[turn, row] = select(col_sum[...], products(tiles))
        backs = back_buf.at[turn]
        back = (n_row, row_peer, lambda other: backs.at[row], backs, row, back_send.at[turn], back_recv.at[turn])
        exchange(*back)
        local = -lin[...] - diag[...] * xs[...]
        arrive(*back)
        residual = local + sum(back_buf[turn, k] for k in range(n_row))

        square = residual * residual
        norm = jnp.sum(square, axis=0, keepdims=True)
        bend = jnp.sum((diag[...] + sigma) * square, axis=0, keepdims=True)
        stages = forward(residual, [norm, bend], turn + 1)
        next(stages)
        next(stages)
        norm, bend = next(stages)
        next(stages)
        arrive(*norms(turn))
        bend = bend + rho * jnp.sum(norm_buf[turn], axis=0)

        step = jnp.sum(norm, axis=1, keepdims=True) / jnp.sum(bend, axis=1, keepdims=True)
        x_now = xs[...]
        xs[...] = relax * (x_now + step * residual) + (1.0 - relax) * x_now
        for k in range(n_lo):
            old = image[k]
            moved = old + step * ag_buf[turn + 1, k]
            image[k] = relax * moved + (1.0 - relax) * old
            mixed = relax * moved + (1.0 - relax) * zs[k]
            y_now = ys[k]
            z_new = jnp.minimum(jnp.maximum(mixed + y_now / rho, low[k]), high[k])
            ys[k] = y_now + rho * (mixed - z_new)
            zs[k] = z_new
        return carry

    lax.fori_loop(0, ITERS, iteration, 0)

    for k in range(n_lo):
        out[k * piece : (k + 1) * piece, :] = zs[k, 0:piece, :]
        out[zb + k * piece : zb + (k + 1) * piece, :] = ys[k, 0:piece, :]
    mine = pltpu.roll(xs[...], lax.rem(lanes - width * row, lanes), axis=1)
    mine = jnp.concatenate([mine, jnp.zeros((lanes - xb, lanes), F32)], axis=0)
    out[2 * zb : 2 * zb + width, :] = mine.T[:width]


def unpack(packed, x_out, z_out, y_out, x_buf, sems):
    zb = z_out.shape[0]
    width, xb = x_out.shape
    copies = (
        pltpu.make_async_copy(packed.at[pl.ds(0, zb)], z_out, sems.at[0]),
        pltpu.make_async_copy(packed.at[pl.ds(zb, zb)], y_out, sems.at[1]),
        pltpu.make_async_copy(x_buf, x_out, sems.at[2]),
    )
    copies[0].start()
    copies[1].start()
    x_buf[...] = packed[2 * zb : 2 * zb + width, :xb]
    copies[2].start()
    for copy in copies:
        copy.wait()


def solution(mesh):
    n_row, n_col = mesh.shape["row"], mesh.shape["col"]
    n_lo = 8
    n_hi = n_col // n_lo

    def shards(values, rows, cols, x0, z0, y0, low0, high0, diag0, lin0, rho, sigma, relax):
        order = values.shape[-1]
        tiles = values.reshape(-1, order, order)
        count = tiles.shape[0]
        zb, lanes = z0.shape
        xb, width = x0.shape
        piece = zb // n_lo
        pad = (piece + 2 + 7) // 8 * 8
        dims = (n_row, n_hi, n_lo, xb, zb, pad, width)
        smem = pltpu.SMEM
        vmem = pltpu.VMEM
        dma = pltpu.SemaphoreType.DMA
        wide = (n_lo, pad, lanes)
        packed = pl.pallas_call(
            functools.partial(kernel, dims),
            out_shape=vmem((2 * zb + width, lanes), F32),
            in_specs=[pl.BlockSpec(memory_space=smem)] * 3 + [pl.BlockSpec(memory_space=pl.ANY)] * 10,
            out_specs=pl.BlockSpec(memory_space=pltpu.VMEM),
            scratch_shapes=[
                smem((1, count), jnp.int32),
                smem((1, count), jnp.int32),
                vmem((2, 1, count), jnp.int32),
                vmem((3, width, xb), F32),
                vmem((4, zb, lanes), F32),
                vmem((count, order, order), F32),
                vmem((count, order, order), F32),
                vmem((count, lanes), F32),
                vmem((count, lanes), F32),
                vmem((n_lo * pad, lanes), F32),
                vmem((n_lo * pad, count), BF16),
                vmem((xb, count), BF16),
                *[vmem(wide, F32)] * 5,
                *[vmem((xb, lanes), F32)] * 3,
                vmem((n_row, width, lanes), F32),
                vmem((n_row, 2, width, lanes), F32),
                vmem((ITERS, n_row, xb, lanes), F32),
                vmem((ITERS + 1, *wide), F32),
                vmem((ITERS + 1, *wide), F32),
                vmem((ITERS + 1, n_hi, pad, lanes), F32),
                vmem((ITERS + 1, *wide), F32),
                vmem((ITERS, n_row * n_lo, 1, lanes), F32),
                dma((6,)),
                dma(()),
                dma(()),
                dma(()),
                dma(()),
                dma((ITERS,)),
                dma((ITERS,)),
                *[dma((ITERS + 1,))] * 6,
                dma((ITERS,)),
                dma((ITERS,)),
            ],
            compiler_params=pltpu.CompilerParams(collective_id=0, has_side_effects=True),
            name="admm",
        )(
            rho, sigma, relax, rows.reshape(1, -1), cols.reshape(1, -1),
            x0.T, diag0.T, lin0.T, z0, y0, low0, high0, tiles,
        )
        x_new, z_new, y_new = pl.pallas_call(
            unpack,
            in_specs=[pl.BlockSpec(memory_space=vmem)],
            out_specs=(pl.BlockSpec(memory_space=pl.ANY),) * 3,
            scratch_shapes=[vmem((width, xb), F32), dma((3,))],
            out_shape=(
                jax.ShapeDtypeStruct((width, xb), F32),
                jax.ShapeDtypeStruct((zb, lanes), F32),
                jax.ShapeDtypeStruct((zb, lanes), F32),
            ),
            name="unpack",
        )(pltpu.with_memory_space_constraint(packed, vmem))
        return x_new.T, z_new, y_new

    placed = (
        P("row", "col", None, None, None),
        P("row", "col", None),
        P("row", "col", None),
        P("col", "row"),
        P("row", None),
        P("row", None),
        P("row", None),
        P("row", None),
        P("col", "row"),
        P("col", "row"),
        P(),
        P(),
        P(),
    )
    return jax.shard_map(
        shards,
        mesh=mesh,
        in_specs=placed,
        out_specs=(P("col", "row"), P("row", None), P("row", None)),
        check_vma=False,
    )
```

```python
import functools

import jax
import jax.numpy as jnp
from jax import lax
from jax.experimental import pallas as pl
from jax.experimental.pallas import tpu as pltpu
from jax.sharding import PartitionSpec as P

ITERS = 2
ON_MXU = 48
MESH = pl.DeviceIdType.MESH
F32 = jnp.float32
BF16 = jnp.bfloat16


def pieces(value, count):
    out = []
    for _ in range(count - 1):
        head = value.astype(BF16)
        out.append(head)
        value = value - head.astype(F32)
    out.append(value.astype(BF16))
    return out


def select(table, value):
    return sum(jnp.dot(table, part, preferred_element_type=F32) for part in pieces(value, 2))


def kernel(
    dims,
    rho_ref,
    sigma_ref,
    relax_ref,
    rows_hbm,
    cols_hbm,
    x0_hbm,
    diag0_hbm,
    lin0_hbm,
    z0_hbm,
    y0_hbm,
    low0_hbm,
    high0_hbm,
    tiles_hbm,
    out,
    rows_ref,
    cols_ref,
    index_buf,
    small_buf,
    plain_buf,
    tiles,
    turned,
    forward_weights,
    backward_weights,
    acc,
    picked,
    vector_buf,
    row_sum,
    col_sum,
    zs,
    ys,
    low,
    high,
    image,
    xs,
    diag,
    lin,
    start_buf,
    cost_buf,
    back_buf,
    part_buf,
    rs_buf,
    ar_buf,
    ag_buf,
    norm_buf,
    load_sem,
    start_send,
    start_recv,
    cost_send,
    cost_recv,
    back_send,
    back_recv,
    rs_send,
    rs_recv,
    ar_send,
    ar_recv,
    ag_send,
    ag_recv,
    norm_send,
    norm_recv,
):
    n_row, n_hi, n_lo, xb, zb, pad, width = dims
    count = tiles.shape[0]
    lanes = tiles.shape[2]
    piece = zb // n_lo
    row = lax.axis_index("row")
    col = lax.axis_index("col")
    hi = lax.div(col, n_lo)
    lo = lax.rem(col, n_lo)

    def row_peer(step):
        other = lax.rem(row + step, n_row)
        return other, (other, col)

    def hi_peer(step):
        other = lax.rem(hi + step, n_hi)
        return other, (row, other * n_lo + lo)

    def lo_peer(step):
        other = lax.rem(lo + step, n_lo)
        return other, (row, hi * n_lo + other)

    far = sorted(((a, b) for a in range(n_row) for b in range(n_lo)), key=lambda s: abs(s[0] - n_row / 2) + abs(s[1] - n_lo / 2))

    def plane_peer(step):
        other_row = lax.rem(row + far[step - 1][0], n_row)
        other_lo = lax.rem(lo + far[step - 1][1], n_lo)
        return other_row * n_lo + other_lo, (other_row, hi * n_lo + other_lo)

    n_plane = n_row * n_lo
    plane = row * n_lo + lo

    barrier = pltpu.get_barrier_semaphore()
    for size, peer in ((n_plane, plane_peer), (n_hi, hi_peer)):
        for step in range(1, size):
            pl.semaphore_signal(barrier, inc=1, device_id=peer(step)[1], device_id_type=MESH)

    smalls = [(x0_hbm, small_buf.at[0], 0), (diag0_hbm, small_buf.at[1], 0), (lin0_hbm, small_buf.at[2], 0)]
    indices = [(rows_hbm, index_buf.at[0], 1), (cols_hbm, index_buf.at[1], 1), (rows_hbm, rows_ref, 2), (cols_hbm, cols_ref, 3)]
    plains = [(ref, plain_buf.at[k], 4) for k, ref in enumerate((z0_hbm, y0_hbm, low0_hbm, high0_hbm))]
    for source, target, k in [*smalls, *indices, *plains, (tiles_hbm, tiles, 5)]:
        pltpu.make_async_copy(source, target, load_sem.at[k]).start()

    def loaded(k, target):
        pltpu.make_async_copy(target, target, load_sem.at[k]).wait()

    def exchange(size, peer, source, buffer, mine, send_sem, recv_sem):
        for step in range(1, size):
            other, device = peer(step)
            pltpu.make_async_remote_copy(
                src_ref=source(other),
                dst_ref=buffer.at[mine],
                send_sem=send_sem,
                recv_sem=recv_sem,
                device_id=device,
                device_id_type=MESH,
            ).start()

    def arrive(size, peer, source, buffer, mine, send_sem, recv_sem):
        every = buffer.at[pl.ds(0, size - 1)]
        copies = pltpu.make_async_remote_copy(
            src_ref=every,
            dst_ref=every,
            send_sem=send_sem,
            recv_sem=recv_sem,
            device_id=peer(1)[1],
            device_id_type=MESH,
        )
        copies.wait_recv()
        copies.wait_send()

    def weigh(weights, tile_of):
        for k in range(ON_MXU):
            heads, rest = pieces(tile_of(k), 2)
            side = slice(lanes * (k % 2), lanes * (k % 2 + 1))
            weights[k // 2, 0:lanes, side] = heads
            weights[k // 2, lanes : 2 * lanes, side] = rest

    empty = jnp.zeros((width, lanes - xb), F32)
    loaded(0, small_buf)
    loaded(1, index_buf)
    start_buf[row] = jnp.concatenate([small_buf[0], empty], axis=1)
    for k in range(2):
        cost_buf[row, k] = jnp.concatenate([small_buf[k + 1], empty], axis=1)

    rows = index_buf[0]
    padded = rows
    for k in range(1, n_lo):
        padded = padded + jnp.where(rows >= k * piece, pad - piece, 0)
    row_sum[...] = (lax.broadcasted_iota(jnp.int32, (n_lo * pad, count), 0) == padded).astype(BF16)
    col_sum[...] = (lax.broadcasted_iota(jnp.int32, (xb, count), 0) == index_buf[1]).astype(BF16)
    loaded(2, rows_ref)
    loaded(3, cols_ref)

    pl.semaphore_wait(barrier, n_plane - 1 + n_hi - 1)

    start = (n_row, row_peer, lambda other: start_buf.at[row], start_buf, row, start_send, start_recv)
    exchange(*start)
    cost = (n_row, row_peer, lambda other: cost_buf.at[row], cost_buf, row, cost_send, cost_recv)
    exchange(*cost)

    loaded(4, plain_buf)
    loaded(5, tiles)
    weigh(forward_weights, lambda k: tiles[k].T)
    for k in range(ON_MXU, count):
        turned[k - ON_MXU] = tiles[k].T
    for index, ref in enumerate((zs, ys, low, high)):
        for k in range(n_lo):
            ref[k] = plain_buf[index, k * piece : (k + 1) * piece, :]

    rho = rho_ref[0]
    sigma = sigma_ref[0]
    relax = relax_ref[0]

    def products(weights, plain):
        vectors = picked[...]
        none = jnp.zeros((8, lanes), F32)
        for first in range(0, ON_MXU, 8):
            vector = vectors[first : first + 8]
            heads = vector.astype(BF16).astype(F32)
            top = jnp.concatenate([heads, heads], axis=1)
            bottom = jnp.concatenate([vector - heads, none], axis=1)
            left = jnp.concatenate([top, bottom], axis=0).astype(BF16)
            for k in range(0, 8, 2):
                both = jnp.dot(left, weights[(first + k) // 2], preferred_element_type=F32)
                both = both[:8] + both[8:]
                acc[first + k : first + k + 1, :] = both[k : k + 1, :lanes]
                acc[first + k + 1 : first + k + 2, :] = both[k + 1 : k + 2, lanes:]
        columns = vectors.T
        for k in range(ON_MXU, count):
            terms = plain(k) * columns[:, k : k + 1]
            acc[k : k + 1, :] = jnp.sum(terms, axis=0, keepdims=True)
        return acc[...]

    def forward(vector, scalars, turn):
        vector_buf[0:xb, :] = vector
        for k in range(count):
            picked[k : k + 1, :] = vector_buf[pl.ds(cols_ref[0, k], 1), :]
        part = select(row_sum[...], products(forward_weights, lambda k: turned[k - ON_MXU]))
        part_buf[turn] = part.reshape(n_lo, pad, lanes)
        for k, value in enumerate(scalars):
            for slot in range(n_lo):
                part_buf[turn, slot, piece + k : piece + k + 1, :] = value
        rs_buf[turn, lo] = part_buf[turn, lo]
        used = pl.ds(0, piece + len(scalars))
        parts = part_buf.at[turn, :, used]
        landed = rs_buf.at[turn, :, used]
        scatter = (n_lo, lo_peer, lambda other: parts.at[other], landed, lo, rs_send.at[turn], rs_recv.at[turn])
        exchange(*scatter)
        yield
        arrive(*scatter)
        sums = ar_buf.at[turn, :, used]
        sums[hi] = sum(landed[k] for k in range(n_lo))
        reduce = (n_hi, hi_peer, lambda other: sums.at[hi], sums, hi, ar_send.at[turn], ar_recv.at[turn])
        exchange(*reduce)
        yield
        arrive(*reduce)
        whole = sum(sums[k] for k in range(n_hi))
        kept = whole[:piece]
        wholes = ag_buf.at[turn, :, pl.ds(0, piece)]
        wholes[lo] = kept
        gather = (n_lo, lo_peer, lambda other: wholes.at[lo], wholes, lo, ag_send.at[turn], ag_recv.at[turn])
        exchange(*gather)
        if scalars:
            norm_buf[turn - 1, plane] = jnp.sum(kept * kept, axis=0, keepdims=True)
            exchange(*norms(turn - 1))
        yield [whole[piece + k : piece + k + 1, :] for k in range(len(scalars))]
        arrive(*gather)
        yield

    def norms(turn):
        buffer = norm_buf.at[turn]
        return n_plane, plane_peer, lambda other: buffer.at[plane], buffer, plane, norm_send.at[turn], norm_recv.at[turn]

    arrive(*start)
    xs[...] = jnp.concatenate([start_buf[k] for k in range(n_row)], axis=0).T[:xb]
    stages = forward(xs[...], [], 0)
    next(stages)
    weigh(backward_weights, lambda k: tiles[k])
    arrive(*cost)
    diag[...] = jnp.concatenate([cost_buf[k, 0] for k in range(n_row)], axis=0).T[:xb]
    lin[...] = jnp.concatenate([cost_buf[k, 1] for k in range(n_row)], axis=0).T[:xb]
    for _ in stages:
        pass
    for k in range(n_lo):
        image[k] = ag_buf[0, k, 0:piece, :]

    def iteration(turn, carry):
        for k in range(n_lo):
            vector_buf[k * pad : k * pad + piece, :] = rho * zs[k] - ys[k] - rho * image[k]
        for k in range(count):
            index = rows_ref[0, k]
            index = index + (pad - piece) * (index // piece)
            picked[k : k + 1, :] = vector_buf[pl.ds(index, 1), :]
        back_buf[turn, row] = select(col_sum[...], products(backward_weights, lambda k: tiles[k]))
        backs = back_buf.at[turn]
        back = (n_row, row_peer, lambda other: backs.at[row], backs, row, back_send.at[turn], back_recv.at[turn])
        exchange(*back)
        local = -lin[...] - diag[...] * xs[...]
        arrive(*back)
        residual = local + sum(back_buf[turn, k] for k in range(n_row))

        square = residual * residual
        norm = jnp.sum(square, axis=0, keepdims=True)
        bend = jnp.sum((diag[...] + sigma) * square, axis=0, keepdims=True)
        stages = forward(residual, [norm, bend], turn + 1)
        next(stages)
        next(stages)
        norm, bend = next(stages)
        next(stages)
        arrive(*norms(turn))
        bend = bend + rho * jnp.sum(norm_buf[turn], axis=0)

        step = jnp.sum(norm, axis=1, keepdims=True) / jnp.sum(bend, axis=1, keepdims=True)
        x_now = xs[...]
        xs[...] = relax * (x_now + step * residual) + (1.0 - relax) * x_now
        for k in range(n_lo):
            old = image[k]
            moved = old + step * ag_buf[turn + 1, k, 0:piece, :]
            image[k] = relax * moved + (1.0 - relax) * old
            mixed = relax * moved + (1.0 - relax) * zs[k]
            y_now = ys[k]
            z_new = jnp.minimum(jnp.maximum(mixed + y_now / rho, low[k]), high[k])
            ys[k] = y_now + rho * (mixed - z_new)
            zs[k] = z_new
        return carry

    lax.fori_loop(0, ITERS, iteration, 0)

    for k in range(n_lo):
        out[k * piece : (k + 1) * piece, :] = zs[k]
        out[zb + k * piece : zb + (k + 1) * piece, :] = ys[k]
    mine = pltpu.roll(xs[...], lax.rem(lanes - width * row, lanes), axis=1)
    mine = jnp.concatenate([mine, jnp.zeros((lanes - xb, lanes), F32)], axis=0)
    out[2 * zb : 2 * zb + width, :] = mine.T[:width]


def unpack(packed, x_out, z_out, y_out, x_buf, sems):
    zb = z_out.shape[0]
    width, xb = x_out.shape
    copies = (
        pltpu.make_async_copy(packed.at[pl.ds(0, zb)], z_out, sems.at[0]),
        pltpu.make_async_copy(packed.at[pl.ds(zb, zb)], y_out, sems.at[1]),
        pltpu.make_async_copy(x_buf, x_out, sems.at[2]),
    )
    copies[0].start()
    copies[1].start()
    x_buf[...] = packed[2 * zb : 2 * zb + width, :xb]
    copies[2].start()
    for copy in copies:
        copy.wait()


def solution(mesh):
    n_row, n_col = mesh.shape["row"], mesh.shape["col"]
    n_lo = 8
    n_hi = n_col // n_lo

    def shards(values, rows, cols, x0, z0, y0, low0, high0, diag0, lin0, rho, sigma, relax):
        order = values.shape[-1]
        tiles = values.reshape(-1, order, order)
        count = tiles.shape[0]
        zb, lanes = z0.shape
        xb, width = x0.shape
        piece = zb // n_lo
        pad = (piece + 2 + 7) // 8 * 8
        dims = (n_row, n_hi, n_lo, xb, zb, pad, width)
        smem = pltpu.SMEM
        vmem = pltpu.VMEM
        dma = pltpu.SemaphoreType.DMA
        wide = (n_lo, pad, lanes)
        packed = pl.pallas_call(
            functools.partial(kernel, dims),
            out_shape=vmem((2 * zb + width, lanes), F32),
            in_specs=[pl.BlockSpec(memory_space=smem)] * 3 + [pl.BlockSpec(memory_space=pl.ANY)] * 10,
            out_specs=pl.BlockSpec(memory_space=pltpu.VMEM),
            scratch_shapes=[
                smem((1, count), jnp.int32),
                smem((1, count), jnp.int32),
                vmem((2, 1, count), jnp.int32),
                vmem((3, width, xb), F32),
                vmem((4, zb, lanes), F32),
                vmem((count, order, order), F32),
                vmem((count - ON_MXU, order, order), F32),
                vmem((ON_MXU // 2, 2 * order, 2 * order), BF16),
                vmem((ON_MXU // 2, 2 * order, 2 * order), BF16),
                vmem((count, lanes), F32),
                vmem((count, lanes), F32),
                vmem((n_lo * pad, lanes), F32),
                vmem((n_lo * pad, count), BF16),
                vmem((xb, count), BF16),
                *[vmem((n_lo, piece, lanes), F32)] * 5,
                *[vmem((xb, lanes), F32)] * 3,
                vmem((n_row, width, lanes), F32),
                vmem((n_row, 2, width, lanes), F32),
                vmem((ITERS, n_row, xb, lanes), F32),
                vmem((ITERS + 1, *wide), F32),
                vmem((ITERS + 1, *wide), F32),
                vmem((ITERS + 1, n_hi, pad, lanes), F32),
                vmem((ITERS + 1, *wide), F32),
                vmem((ITERS, n_row * n_lo, 1, lanes), F32),
                dma((6,)),
                dma(()),
                dma(()),
                dma(()),
                dma(()),
                dma((ITERS,)),
                dma((ITERS,)),
                *[dma((ITERS + 1,))] * 6,
                dma((ITERS,)),
                dma((ITERS,)),
            ],
            compiler_params=pltpu.CompilerParams(collective_id=0, has_side_effects=True),
            name="admm",
        )(
            rho, sigma, relax, rows.reshape(1, -1), cols.reshape(1, -1),
            x0.T, diag0.T, lin0.T, z0, y0, low0, high0, tiles,
        )
        x_new, z_new, y_new = pl.pallas_call(
            unpack,
            in_specs=[pl.BlockSpec(memory_space=vmem)],
            out_specs=(pl.BlockSpec(memory_space=pl.ANY),) * 3,
            scratch_shapes=[vmem((width, xb), F32), dma((3,))],
            out_shape=(
                jax.ShapeDtypeStruct((width, xb), F32),
                jax.ShapeDtypeStruct((zb, lanes), F32),
                jax.ShapeDtypeStruct((zb, lanes), F32),
            ),
            name="unpack",
        )(pltpu.with_memory_space_constraint(packed, vmem))
        return x_new.T, z_new, y_new

    placed = (
        P("row", "col", None, None, None),
        P("row", "col", None),
        P("row", "col", None),
        P("col", "row"),
        P("row", None),
        P("row", None),
        P("row", None),
        P("row", None),
        P("col", "row"),
        P("col", "row"),
        P(),
        P(),
        P(),
    )
    return jax.shard_map(
        shards,
        mesh=mesh,
        in_specs=placed,
        out_specs=(P("col", "row"), P("row", None), P("row", None)),
        check_vma=False,
    )
```

```python
import functools

import jax
import jax.numpy as jnp
from jax import lax
from jax.experimental import pallas as pl
from jax.experimental.pallas import tpu as pltpu
from jax.sharding import PartitionSpec as P

ITERS = 2
ON_MXU = 48
MESH = pl.DeviceIdType.MESH
F32 = jnp.float32
BF16 = jnp.bfloat16


def pieces(value, count):
    out = []
    for _ in range(count - 1):
        head = value.astype(BF16)
        out.append(head)
        value = value - head.astype(F32)
    out.append(value.astype(BF16))
    return out


def select(table, value):
    return sum(jnp.dot(table, part, preferred_element_type=F32) for part in pieces(value, 2))


def kernel(
    dims,
    rho_ref,
    sigma_ref,
    relax_ref,
    rows_hbm,
    cols_hbm,
    x0_hbm,
    diag0_hbm,
    lin0_hbm,
    z0_hbm,
    y0_hbm,
    low0_hbm,
    high0_hbm,
    tiles_hbm,
    out,
    rows_ref,
    cols_ref,
    places_ref,
    index_buf,
    small_buf,
    plain_buf,
    tiles,
    turned,
    forward_weights,
    backward_weights,
    acc,
    picked,
    vector_buf,
    row_sum,
    col_sum,
    zs,
    ys,
    low,
    high,
    image,
    xs,
    diag,
    lin,
    start_buf,
    cost_buf,
    back_buf,
    part_buf,
    rs_buf,
    ar_buf,
    ag_buf,
    norm_buf,
    load_sem,
    start_send,
    start_recv,
    cost_send,
    cost_recv,
    back_send,
    back_recv,
    rs_send,
    rs_recv,
    ar_send,
    ar_recv,
    ag_send,
    ag_recv,
    norm_send,
    norm_recv,
):
    n_row, n_hi, n_lo, xb, zb, pad, width = dims
    count = tiles.shape[0]
    lanes = tiles.shape[2]
    piece = zb // n_lo
    row = lax.axis_index("row")
    col = lax.axis_index("col")
    hi = lax.div(col, n_lo)
    lo = lax.rem(col, n_lo)

    def away(size):
        return sorted(range(size), key=lambda k: -min(k, size - k))

    pairs = [(a, b) for a in away(n_row // 2) for b in (1, 0)]

    def moved(place, pair):
        outer, inner = lax.div(place, 2), lax.rem(place, 2)
        return lax.rem(outer + pair[0], n_row // 2) * 2 + (1 - inner if pair[1] else inner)

    def row_peer(step):
        other = moved(row, pairs[step - 1])
        return other, (other, col)

    def hi_peer(step):
        other = lax.rem(hi + away(n_hi)[step - 1], n_hi)
        return other, (row, other * n_lo + lo)

    def lo_peer(step):
        other = moved(lo, pairs[step - 1])
        return other, (row, hi * n_lo + other)

    def hops(pair):
        return min(pair[0], n_row // 2 - pair[0]) + 0.5 * pair[1]

    planes = sorted(((a, b) for a in pairs for b in pairs), key=lambda ab: -hops(ab[0]) - hops(ab[1]))

    def plane_peer(step):
        other_row, other_lo = moved(row, planes[step - 1][0]), moved(lo, planes[step - 1][1])
        return other_row * n_lo + other_lo, (other_row, hi * n_lo + other_lo)

    n_plane = n_row * n_lo
    plane = row * n_lo + lo

    smalls = [(x0_hbm, small_buf.at[0], 0), (diag0_hbm, small_buf.at[1], 0), (lin0_hbm, small_buf.at[2], 0)]
    indices = [(rows_hbm, index_buf.at[0], 1), (cols_hbm, index_buf.at[1], 1), (rows_hbm, rows_ref, 2), (cols_hbm, cols_ref, 3)]
    plains = [(ref, plain_buf.at[k], 4) for k, ref in enumerate((z0_hbm, y0_hbm, low0_hbm, high0_hbm))]
    for source, target, k in [*smalls, *indices, *plains, (tiles_hbm, tiles, 5)]:
        pltpu.make_async_copy(source, target, load_sem.at[k]).start()

    barrier = pltpu.get_barrier_semaphore()
    for size, peer in ((n_row, row_peer), (n_lo, lo_peer), (n_hi, hi_peer)):
        for step in range(1, size):
            pl.semaphore_signal(barrier, inc=1, device_id=peer(step)[1], device_id_type=MESH)

    def loaded(k, target):
        pltpu.make_async_copy(target, target, load_sem.at[k]).wait()

    def exchange(size, peer, source, buffer, mine, send_sem, recv_sem):
        for step in range(1, size):
            other, device = peer(step)
            pltpu.make_async_remote_copy(
                src_ref=source(other),
                dst_ref=buffer.at[mine],
                send_sem=send_sem,
                recv_sem=recv_sem,
                device_id=device,
                device_id_type=MESH,
            ).start()

    def arrive(size, peer, source, buffer, mine, send_sem, recv_sem):
        every = buffer.at[pl.ds(0, size - 1)]
        copies = pltpu.make_async_remote_copy(
            src_ref=every,
            dst_ref=every,
            send_sem=send_sem,
            recv_sem=recv_sem,
            device_id=peer(1)[1],
            device_id_type=MESH,
        )
        copies.wait_recv()
        copies.wait_send()

    def weigh(weights, tile_of):
        for k in range(ON_MXU):
            heads, rest = pieces(tile_of(k), 2)
            side = slice(lanes * (k % 2), lanes * (k % 2 + 1))
            weights[k // 2, 0:lanes, side] = heads
            weights[k // 2, lanes : 2 * lanes, side] = rest

    loaded(0, small_buf)
    empty = jnp.zeros((width, lanes - xb), F32)
    start_buf[row] = jnp.concatenate([small_buf[0], empty], axis=1)
    for k in range(2):
        cost_buf[row, k] = jnp.concatenate([small_buf[k + 1], empty], axis=1)

    pl.semaphore_wait(barrier, n_row + n_lo + n_hi - 3)

    start = (n_row, row_peer, lambda other: start_buf.at[row], start_buf, row, start_send, start_recv)
    exchange(*start)
    cost = (n_row, row_peer, lambda other: cost_buf.at[row], cost_buf, row, cost_send, cost_recv)
    exchange(*cost)

    loaded(1, index_buf)
    rows = index_buf[0]
    padded = rows
    for k in range(1, n_lo):
        padded = padded + jnp.where(rows >= k * piece, pad - piece, 0)
    row_sum[...] = (lax.broadcasted_iota(jnp.int32, (n_lo * pad, count), 0) == padded).astype(BF16)
    col_sum[...] = (lax.broadcasted_iota(jnp.int32, (xb, count), 0) == index_buf[1]).astype(BF16)
    loaded(2, rows_ref)
    loaded(3, cols_ref)
    for k in range(count):
        index = rows_ref[0, k]
        places_ref[k] = index + (pad - piece) * (index // piece)

    loaded(4, plain_buf)
    loaded(5, tiles)
    weigh(forward_weights, lambda k: tiles[k].T)
    for k in range(ON_MXU, count):
        turned[k - ON_MXU] = tiles[k].T
    for index, ref in enumerate((zs, ys, low, high)):
        for k in range(n_lo):
            ref[k] = plain_buf[index, k * piece : (k + 1) * piece, :]

    rho = rho_ref[0]
    sigma = sigma_ref[0]
    relax = relax_ref[0]

    def products(weights, plain):
        vectors = picked[...]
        none = jnp.zeros((8, lanes), F32)
        for first in range(0, ON_MXU, 8):
            vector = vectors[first : first + 8]
            heads = vector.astype(BF16).astype(F32)
            top = jnp.concatenate([heads, heads], axis=1)
            bottom = jnp.concatenate([vector - heads, none], axis=1)
            left = jnp.concatenate([top, bottom], axis=0).astype(BF16)
            for k in range(0, 8, 2):
                both = jnp.dot(left, weights[(first + k) // 2], preferred_element_type=F32)
                both = both[:8] + both[8:]
                acc[first + k : first + k + 1, :] = both[k : k + 1, :lanes]
                acc[first + k + 1 : first + k + 2, :] = both[k + 1 : k + 2, lanes:]
        columns = vectors.T
        for k in range(ON_MXU, count):
            terms = plain(k) * columns[:, k : k + 1]
            acc[k : k + 1, :] = jnp.sum(terms, axis=0, keepdims=True)
        return acc[...]

    def forward(vector, scalars, turn):
        vector_buf[0:xb, :] = vector
        for k in range(count):
            picked[k : k + 1, :] = vector_buf[pl.ds(cols_ref[0, k], 1), :]
        part = select(row_sum[...], products(forward_weights, lambda k: turned[k - ON_MXU]))
        part_buf[turn] = part.reshape(n_lo, pad, lanes)
        for k, value in enumerate(scalars):
            for slot in range(n_lo):
                part_buf[turn, slot, piece + k : piece + k + 1, :] = value
        rs_buf[turn, lo] = part_buf[turn, lo]
        used = pl.ds(0, piece + len(scalars))
        parts = part_buf.at[turn, :, used]
        landed = rs_buf.at[turn, :, used]
        scatter = (n_lo, lo_peer, lambda other: parts.at[other], landed, lo, rs_send.at[turn], rs_recv.at[turn])
        exchange(*scatter)
        yield
        arrive(*scatter)
        sums = ar_buf.at[turn, :, used]
        sums[hi] = sum(landed[k] for k in range(n_lo))
        reduce = (n_hi, hi_peer, lambda other: sums.at[hi], sums, hi, ar_send.at[turn], ar_recv.at[turn])
        exchange(*reduce)
        yield
        arrive(*reduce)
        whole = sum(sums[k] for k in range(n_hi))
        kept = whole[:piece]
        wholes = ag_buf.at[turn, :, pl.ds(0, piece)]
        wholes[lo] = kept
        gather = (n_lo, lo_peer, lambda other: wholes.at[lo], wholes, lo, ag_send.at[turn], ag_recv.at[turn])
        exchange(*gather)
        if scalars:
            norm_buf[turn - 1, plane] = jnp.sum(kept * kept, axis=0, keepdims=True)
            exchange(*norms(turn - 1))
        yield [whole[piece + k : piece + k + 1, :] for k in range(len(scalars))]
        arrive(*gather)
        yield

    def norms(turn):
        buffer = norm_buf.at[turn]
        return n_plane, plane_peer, lambda other: buffer.at[plane], buffer, plane, norm_send.at[turn], norm_recv.at[turn]

    arrive(*start)
    xs[...] = jnp.concatenate([start_buf[k] for k in range(n_row)], axis=0).T[:xb]
    stages = forward(xs[...], [], 0)
    next(stages)
    weigh(backward_weights, lambda k: tiles[k])
    arrive(*cost)
    diag[...] = jnp.concatenate([cost_buf[k, 0] for k in range(n_row)], axis=0).T[:xb]
    lin[...] = jnp.concatenate([cost_buf[k, 1] for k in range(n_row)], axis=0).T[:xb]
    for _ in stages:
        pass
    for k in range(n_lo):
        image[k] = ag_buf[0, k, 0:piece, :]

    def iteration(turn, carry):
        for k in range(n_lo):
            vector_buf[k * pad : k * pad + piece, :] = rho * zs[k] - ys[k] - rho * image[k]
        for k in range(count):
            picked[k : k + 1, :] = vector_buf[pl.ds(places_ref[k], 1), :]
        back_buf[turn, row] = select(col_sum[...], products(backward_weights, lambda k: tiles[k]))
        backs = back_buf.at[turn]
        back = (n_row, row_peer, lambda other: backs.at[row], backs, row, back_send.at[turn], back_recv.at[turn])
        exchange(*back)
        local = -lin[...] - diag[...] * xs[...]
        arrive(*back)
        residual = local + sum(back_buf[turn, k] for k in range(n_row))

        square = residual * residual
        norm = jnp.sum(square, axis=0, keepdims=True)
        bend = jnp.sum((diag[...] + sigma) * square, axis=0, keepdims=True)
        stages = forward(residual, [norm, bend], turn + 1)
        next(stages)
        next(stages)
        norm, bend = next(stages)
        next(stages)
        arrive(*norms(turn))
        bend = bend + rho * jnp.sum(norm_buf[turn], axis=0)

        step = jnp.sum(norm, axis=1, keepdims=True) / jnp.sum(bend, axis=1, keepdims=True)
        x_now = xs[...]
        xs[...] = relax * (x_now + step * residual) + (1.0 - relax) * x_now
        for k in range(n_lo):
            old = image[k]
            moved = old + step * ag_buf[turn + 1, k, 0:piece, :]
            image[k] = relax * moved + (1.0 - relax) * old
            mixed = relax * moved + (1.0 - relax) * zs[k]
            y_now = ys[k]
            z_new = jnp.minimum(jnp.maximum(mixed + y_now / rho, low[k]), high[k])
            ys[k] = y_now + rho * (mixed - z_new)
            zs[k] = z_new
        return carry

    lax.fori_loop(0, ITERS, iteration, 0)

    for k in range(n_lo):
        out[k * piece : (k + 1) * piece, :] = zs[k]
        out[zb + k * piece : zb + (k + 1) * piece, :] = ys[k]
    mine = pltpu.roll(xs[...], lax.rem(lanes - width * row, lanes), axis=1)
    mine = jnp.concatenate([mine, jnp.zeros((lanes - xb, lanes), F32)], axis=0)
    out[2 * zb : 2 * zb + width, :] = mine.T[:width]


def unpack(packed, x_out, z_out, y_out, x_buf, sems):
    zb = z_out.shape[0]
    width, xb = x_out.shape
    copies = (
        pltpu.make_async_copy(packed.at[pl.ds(0, zb)], z_out, sems.at[0]),
        pltpu.make_async_copy(packed.at[pl.ds(zb, zb)], y_out, sems.at[1]),
        pltpu.make_async_copy(x_buf, x_out, sems.at[2]),
    )
    copies[0].start()
    copies[1].start()
    x_buf[...] = packed[2 * zb : 2 * zb + width, :xb]
    copies[2].start()
    for copy in copies:
        copy.wait()


def solution(mesh):
    n_row, n_col = mesh.shape["row"], mesh.shape["col"]
    n_lo = 8
    n_hi = n_col // n_lo

    def shards(values, rows, cols, x0, z0, y0, low0, high0, diag0, lin0, rho, sigma, relax):
        order = values.shape[-1]
        tiles = values.reshape(-1, order, order)
        count = tiles.shape[0]
        zb, lanes = z0.shape
        xb, width = x0.shape
        piece = zb // n_lo
        pad = (piece + 2 + 7) // 8 * 8
        dims = (n_row, n_hi, n_lo, xb, zb, pad, width)
        smem = pltpu.SMEM
        vmem = pltpu.VMEM
        dma = pltpu.SemaphoreType.DMA
        wide = (n_lo, pad, lanes)
        packed = pl.pallas_call(
            functools.partial(kernel, dims),
            out_shape=vmem((2 * zb + width, lanes), F32),
            in_specs=[pl.BlockSpec(memory_space=smem)] * 3 + [pl.BlockSpec(memory_space=pl.ANY)] * 10,
            out_specs=pl.BlockSpec(memory_space=pltpu.VMEM),
            scratch_shapes=[
                smem((1, count), jnp.int32),
                smem((1, count), jnp.int32),
                smem((count,), jnp.int32),
                vmem((2, 1, count), jnp.int32),
                vmem((3, width, xb), F32),
                vmem((4, zb, lanes), F32),
                vmem((count, order, order), F32),
                vmem((count - ON_MXU, order, order), F32),
                vmem((ON_MXU // 2, 2 * order, 2 * order), BF16),
                vmem((ON_MXU // 2, 2 * order, 2 * order), BF16),
                vmem((count, lanes), F32),
                vmem((count, lanes), F32),
                vmem((n_lo * pad, lanes), F32),
                vmem((n_lo * pad, count), BF16),
                vmem((xb, count), BF16),
                *[vmem((n_lo, piece, lanes), F32)] * 5,
                *[vmem((xb, lanes), F32)] * 3,
                vmem((n_row, width, lanes), F32),
                vmem((n_row, 2, width, lanes), F32),
                vmem((ITERS, n_row, xb, lanes), F32),
                vmem((ITERS + 1, *wide), F32),
                vmem((ITERS + 1, *wide), F32),
                vmem((ITERS + 1, n_hi, pad, lanes), F32),
                vmem((ITERS + 1, *wide), F32),
                vmem((ITERS, n_row * n_lo, 1, lanes), F32),
                dma((6,)),
                dma(()),
                dma(()),
                dma(()),
                dma(()),
                dma((ITERS,)),
                dma((ITERS,)),
                *[dma((ITERS + 1,))] * 6,
                dma((ITERS,)),
                dma((ITERS,)),
            ],
            compiler_params=pltpu.CompilerParams(collective_id=0, has_side_effects=True),
            name="admm",
        )(
            rho, sigma, relax, rows.reshape(1, -1), cols.reshape(1, -1),
            x0.T, diag0.T, lin0.T, z0, y0, low0, high0, tiles,
        )
        x_new, z_new, y_new = pl.pallas_call(
            unpack,
            in_specs=[pl.BlockSpec(memory_space=vmem)],
            out_specs=(pl.BlockSpec(memory_space=pl.ANY),) * 3,
            scratch_shapes=[vmem((width, xb), F32), dma((3,))],
            out_shape=(
                jax.ShapeDtypeStruct((width, xb), F32),
                jax.ShapeDtypeStruct((zb, lanes), F32),
                jax.ShapeDtypeStruct((zb, lanes), F32),
            ),
            name="unpack",
        )(pltpu.with_memory_space_constraint(packed, vmem))
        return x_new.T, z_new, y_new

    placed = (
        P("row", "col", None, None, None),
        P("row", "col", None),
        P("row", "col", None),
        P("col", "row"),
        P("row", None),
        P("row", None),
        P("row", None),
        P("row", None),
        P("col", "row"),
        P("col", "row"),
        P(),
        P(),
        P(),
    )
    return jax.shard_map(
        shards,
        mesh=mesh,
        in_specs=placed,
        out_specs=(P("col", "row"), P("row", None), P("row", None)),
        check_vma=False,
    )
```
